32 devices in a mesh: ep: 8 (over z, x), tp: 4 (over y, core).
Axes of the slice: x: 2, y: 2, z: 4, core: 2. Of those that a mesh axis runs over, the one named last changes fastest.
Arguments:
- tokens: bfloat16 [2048, 2048], P('ep', 'tp'), may hold values from -180 to 180
- norm_gain: float32 [2048], replicated, may hold values from 0.1 to 1.9
- router_weight: bfloat16 [2048, 60], P('tp'), may hold values from -2 to 2
- shared_gate_w: bfloat16 [2048], replicated, may hold values from -0.125 to 0.125
- expert_ids: int32 [2048, 4], P('ep'), may hold values from 0 to 59, all different within a row; in each aligned block of 256 rows (0 to 255, 256 to 511, ...) at most 32 rows name the same one
- w_gate: bfloat16 [64, 2048, 1408], P('ep', None, 'tp'), may hold values from -0.125 to 0.125
- w_up: bfloat16 [64, 2048, 1408], P('ep', None, 'tp'), may hold values from -0.125 to 0.125
- w_down: bfloat16 [64, 1408, 2048], P('ep', 'tp'), may hold values from -1.5 to 1.5
- shared_w_gate: bfloat16 [2048, 2816], P(None, 'tp'), may hold values from -0.125 to 0.125
- shared_w_up: bfloat16 [2048, 2816], P(None, 'tp'), may hold values from -0.125 to 0.125
- shared_w_down: bfloat16 [2816, 2048], P('tp'), may hold values from -0.109375 to 0.109375
Outputs:
- moe_out: bfloat16 [2048, 2048], P('ep', 'tp')
The draws below stay inside these ranges and needn't reach their ends.
Inputs may be any that keep to these rules, and one draw needn't show every extreme that they name: `expert_ids`: each row names 4 different experts below 60. Within the 256 rows of one index of ep no expert is named by more than 32 rows, and in some of these blocks one expert is named by exactly 32 rows.
All inputs are finite; a program needn't handle non-finite values.
Results may differ from the reference program's by a relative error of at most 0.0069.
Values may be sent and summed in bfloat16 or wider, within the bound.
A program may use at most 128 MiB of HBM per device.

```python
import math
import jax
import jax.numpy as jnp
import numpy as np
from jax import lax

D = 2048
FE = 1408
EXPERTS = 60
TOPK = 4
SF = 2816
TOK_DEV = 256
CAP = 32
SLOTS = 64
TOKENS = 2048
N_EP = 8


def draw_tokens(key, part):
    base = jax.random.fold_in(key, 11)
    first, second = jax.random.split(base, 2)
    noise = jnp.clip(jax.random.normal(first, (TOKENS, D), jnp.float32), -4.0, 4.0)
    rising = 3.0 ** (jnp.arange(D, dtype=jnp.float32) / D)
    column = jnp.exp(jax.random.uniform(second, (D,), jnp.float32, math.log(0.3), 0.0)) * rising
    values = noise * column[None, :]
    return values.astype(jnp.bfloat16)


def draw_router_weight(key, part):
    base = jax.random.fold_in(key, 13)
    values = jnp.clip(jax.random.normal(base, (D, EXPERTS), jnp.float32), -4.0, 4.0) * (0.4 / math.sqrt(D))
    values = jnp.clip(values, -2.0, 2.0)
    return values.astype(jnp.bfloat16)


def block_levels(key, extent, cuts, low, largest):
    loudness, own = 1.0, jax.random.fold_in(key, 6)
    for dim, shards_of in cuts:
        steps = jnp.exp(jax.random.uniform(jax.random.fold_in(own, dim), (shards_of,), jnp.float32, low / len(cuts), largest / len(cuts)))
        loudness = loudness * jnp.repeat(steps, extent[dim] // shards_of).reshape([-1 if axis == dim else 1 for axis in range(len(extent))])
    return loudness


def deal_out(own_key, own, number, rows, amount, top, most, slope):
    sequence = jax.random.permutation(own_key, amount)
    packed, ordinary = load_shares(amount, rows * top, most, slope, True), load_shares(amount, rows * top, most, slope, False)
    places = jnp.arange(amount)

    def named(lengths, rotation):
        used = int((lengths > 0).sum())
        fixed = max(1, used // 4)
        shifted = fixed + (places - fixed + rotation * (used - fixed)) % max(1, amount - fixed)
        return jnp.zeros((amount,), jnp.int32).at[sequence[jnp.where(places < fixed, places, shifted)]].set(jnp.asarray(lengths, jnp.int32))

    lengths = jnp.where(number % 4 == 0, named(packed, number // 4), named(ordinary, number - number // 4 - 1))
    mixed = jax.random.permutation(jax.random.fold_in(own, 3), amount)
    giver, receiver = mixed[0:amount // 2 * 2:2], mixed[1:amount // 2 * 2:2]
    slack = jnp.minimum(lengths[giver] - 1, most - lengths[receiver]) // 2
    slack = jnp.where((giver == sequence[0]) | (receiver == sequence[0]) | (lengths[receiver] == 0), 0, jnp.maximum(slack, 0))
    shifted = jax.random.randint(jax.random.fold_in(own, 4), (amount // 2,), 0, 1 << 20) % (slack + 1)
    lengths = lengths.at[giver].add(-shifted).at[receiver].add(shifted)
    members = jnp.searchsorted(jnp.cumsum(lengths), jnp.arange(rows * top), side="right").astype(jnp.int32)
    table = members.reshape(top, rows).T
    table = table[jax.random.permutation(jax.random.fold_in(own, 1), rows)]
    rotation = jax.random.randint(jax.random.fold_in(own, 2), (rows, 1), 0, top)
    return jnp.take_along_axis(table, (jnp.arange(top)[None, :] + rotation) % top, axis=1)


def load_shares(amount, total, most, lean, full):
    weights = [(1 << 20) // math.isqrt(rank ** lean) + 1 for rank in range(1, amount + 1)]
    largest = most if full else min(most, max(-(-total // amount), total * weights[0] // sum(weights)))
    least = 1 if total - largest >= amount - 1 else 0
    given, rest = [largest] + [least] * (amount - 1), total - largest - least * (amount - 1)
    while rest > 0:
        free = [i for i in range(1, amount) if given[i] < largest] or [i for i in range(1, amount) if given[i] < most]
        mass, budget = sum([weights[i] for i in free]), rest
        for i in free:
            extra = min(most - given[i], max(1, budget * weights[i] // mass), rest)
            given[i] = given[i] + extra
            rest = rest - extra
    return np.array(given)


def centred(key, shape, scale, reach, cuts=(), kind=jnp.bfloat16):
    values = jax.random.normal(key, shape, jnp.float32) * scale
    if len(cuts) > 0:
        values = block_levels(key, shape, cuts, -0.22, 0.18) * values
    return jnp.clip(values, min=-reach, max=reach).astype(kind)


def setup_inputs(seed: int = 0) -> dict:
    key_list = jax.random.split(jax.random.key(seed), 12)
    tokens = draw_tokens(jax.random.fold_in(key_list[11], 71), 0)
    norm_gain = jnp.clip(1.0 + 0.18 * jax.random.normal(key_list[1], (D,), jnp.float32), 0.1, 1.9)
    router_weight = draw_router_weight(jax.random.fold_in(key_list[11], 71), 0)
    shared_gate_w = centred(key_list[3], (D,), D ** -0.5, 0.125)
    expert_ids_keys = jax.random.split(jax.random.fold_in(key_list[4], 1), TOKENS // TOK_DEV)
    expert_ids_turns = jax.random.permutation(jax.random.fold_in(key_list[4], 3), TOKENS // TOK_DEV)
    expert_ids = jax.vmap(lambda own, number: deal_out(jax.random.fold_in(key_list[4], 2), own, number, TOK_DEV, EXPERTS, TOPK, CAP, 2))(expert_ids_keys, expert_ids_turns).reshape((TOKENS, TOPK))
    w_gate = centred(key_list[5], (SLOTS, D, FE), D ** -0.5, 0.125, ((0, 8), (2, 4)))
    w_up = centred(key_list[6], (SLOTS, D, FE), D ** -0.5, 0.125, ((0, 8), (2, 4)))
    w_down = centred(key_list[7], (SLOTS, FE, D), 0.25, 1.5, ((0, 8), (1, 4)))
    shared_w_gate = centred(key_list[8], (D, SF), D ** -0.5, 0.125, ((1, 4),))
    shared_w_up = centred(key_list[9], (D, SF), D ** -0.5, 0.125, ((1, 4),))
    shared_w_down = centred(key_list[10], (SF, D), SF ** -0.5, 0.109375, ((0, 4),))
    return {"tokens": tokens, "norm_gain": norm_gain, "router_weight": router_weight, "shared_gate_w": shared_gate_w, "expert_ids": expert_ids, "w_gate": w_gate, "w_up": w_up, "w_down": w_down, "shared_w_gate": shared_w_gate, "shared_w_up": shared_w_up, "shared_w_down": shared_w_down}


def reference(tokens, norm_gain, router_weight, shared_gate_w, expert_ids, w_gate, w_up, w_down, shared_w_gate, shared_w_up, shared_w_down):
    values = tokens.astype(jnp.float32)
    inv_rms = lax.rsqrt(lax.optimization_barrier(jnp.mean(values * values, axis=-1, keepdims=True)) + 1e-06)
    normed = (values * inv_rms * norm_gain[None, :]).astype(jnp.bfloat16)
    logits = jnp.dot(normed, router_weight, preferred_element_type=jnp.float32)
    probs = jax.nn.softmax(logits, axis=-1)
    route_weight = jnp.take_along_axis(probs, expert_ids, axis=1)
    shared_gate_act = jnp.dot(normed, shared_w_gate, preferred_element_type=jnp.float32)
    shared_up_act = jnp.dot(normed, shared_w_up, preferred_element_type=jnp.float32)
    shared_hidden = (jax.nn.silu(shared_gate_act) * shared_up_act).astype(jnp.bfloat16)
    shared = jnp.dot(shared_hidden, shared_w_down, preferred_element_type=jnp.float32)
    share_gate = jax.nn.sigmoid(jnp.dot(normed, shared_gate_w, preferred_element_type=jnp.float32))
    assigns = TOKENS * TOPK
    blocked = expert_ids.reshape(N_EP, TOK_DEV * TOPK)
    one_hot = (blocked[:, :, None] == jnp.arange(EXPERTS, dtype=jnp.int32)[None, None, :]).astype(jnp.int32)
    before = jnp.cumsum(one_hot, axis=1) - one_hot
    order_rank = lax.optimization_barrier(jnp.sum(before * one_hot, axis=-1))
    position = jnp.arange(N_EP, dtype=jnp.int32)[:, None] * CAP + order_rank
    assign_ids = jnp.arange(assigns, dtype=jnp.int32)
    table = jnp.full((EXPERTS, N_EP * CAP), assigns, jnp.int32)
    table = table.at[blocked.reshape(-1), position.reshape(-1)].set(assign_ids)
    normed_pad = jnp.concatenate([normed, jnp.zeros((1, D), jnp.bfloat16)], axis=0)
    weight_pad = jnp.concatenate([route_weight.reshape(-1), jnp.zeros((1,), jnp.float32)], axis=0)

    def expert_step(total, expert):
        entries = table[expert]
        token_ids = (entries // TOPK).astype(jnp.int32)
        rows = normed_pad[token_ids]
        gate_act = jnp.dot(rows, w_gate[expert], preferred_element_type=jnp.float32)
        up_act = jnp.dot(rows, w_up[expert], preferred_element_type=jnp.float32)
        hidden = (jax.nn.silu(gate_act) * up_act).astype(jnp.bfloat16)
        result = jnp.dot(hidden, w_down[expert], preferred_element_type=jnp.float32).astype(jnp.bfloat16)
        total = total.at[token_ids].add(weight_pad[entries][:, None] * result.astype(jnp.float32))
        return (total, None)
    routed, _ = lax.scan(expert_step, jnp.zeros((TOKENS + 1, D), jnp.float32), jnp.arange(EXPERTS, dtype=jnp.int32))
    return (share_gate[:, None] * shared + routed[:TOKENS]).astype(jnp.bfloat16)
```

```python
import functools

import jax
import jax.numpy as jnp
from jax import lax
from jax.experimental import pallas as pl
from jax.experimental.pallas import tpu as pltpu
from jax.sharding import PartitionSpec as P

F32 = jnp.float32
BF16 = jnp.bfloat16
MESH = pl.DeviceIdType.MESH


def offsets(nz, order):
    span = {"z": range(-(nz - 1), nz), "x": (0, 1), "y": (0, 1)}
    take = lambda d: span[d] if d in order else (0,)
    return [(a, b, c) for a in take("z") for b in take("x") for c in take("y")]


def last_dim(order, off):
    value = dict(zip("zxy", off))
    return max([i for i, d in enumerate(order) if value[d] != 0], default=-1)


def next_hops(order, off, nz):
    last, dz = last_dim(order, off), off[0]
    hops = []
    for i, d in enumerate(order):
        if d == "z":
            if (last < i or (last == i and dz > 0)) and dz < nz - 1:
                hops.append("u")
            if (last < i or (last == i and dz < 0)) and dz > 1 - nz:
                hops.append("d")
        elif last < i:
            hops.append(d)
    return hops


def moved(off, hop):
    dz, dx, dy = off
    return {
        "u": (dz + 1, dx, dy),
        "d": (dz - 1, dx, dy),
        "x": (dz, 1 - dx, dy),
        "y": (dz, dx, 1 - dy),
    }[hop]


def event_order(nz, streams):
    events = []
    for k, (order, _, n) in enumerate(streams):
        for off in offsets(nz, order):
            value = {"z": abs(off[0]), "x": off[1], "y": off[2]}
            when, load = 0.0, 1
            for d in order:
                when += value[d] * load * n
                load *= nz if d == "z" else 2
            events.append((when, k, off))
    events.sort()
    return [(k, off) for _, k, off in events]


def block_streams(rows):
    part = rows // 16
    cuts = (("zxy", 3 * part), ("zyx", 3 * part), ("xzy", 5 * part), ("yzx", 5 * part))
    streams, start = [], 0
    for order, n in cuts:
        streams.append((order, start, n))
        start += n
    return streams


class Plan:
    def __init__(self, n_ep, rows):
        self.nz = n_ep // 2
        self.streams = block_streams(rows)
        self.extra = [("zx", 0, 1), ("y", 0, 1)]
        every = self.extra + self.streams
        self.events = event_order(self.nz, every)
        self.sends, self.recvs, self.pair = {}, {}, {}
        for k, off in self.events:
            for hop in next_hops(every[k][0], off, self.nz):
                self.sends[k, off, hop] = len(self.sends)
            self.recvs[k, off] = len(self.recvs)
            if k != 0:
                self.pair[k, off] = len(self.pair)
        self.every = every
        self.back = [(k, off) for k, off in reversed(self.events) if k >= 2]
        self.slots, self.slot_rows = {}, 0
        for k, off in self.back:
            for hop in next_hops(every[k][0], off, self.nz):
                self.slots[k, off, hop] = (len(self.slots), self.slot_rows)
                self.slot_rows += every[k][2]
        self.parents = {e: i for i, e in enumerate(self.back)}


def kernel(plan, n_tp, here, experts,
           tok, gain, sgw, rt, ids, wg, wu, wd, swg, swu, swd, out,
           g, xs, pick, sw, pr, part, rbuf, idb, wgb, wub, wdb, sgb, sub, sdb, slot, cbuf,
           loc, wsem, ssem, send, recv, psend, precv, bsend, brecv, bpsend, bprecv):
    nz = plan.nz
    ep, tp = lax.axis_index("ep"), lax.axis_index("tp")
    z, x, y, c = ep // 2, ep % 2, tp // 2, tp % 2
    rows, width = tok.shape
    n_ep = 2 * nz
    cap = rows // 8

    def dev(z_, x_, y_, c_):
        return (z_ * 2 + x_, y_ * 2 + c_)

    to = {
        "u": dev(z + 1, x, y, c),
        "d": dev(z - 1, x, y, c),
        "x": dev(z, 1 - x, y, c),
        "y": dev(z, x, 1 - y, c),
        "c": dev(z, x, y, 1 - c),
    }
    exists = {"u": z < nz - 1, "d": z > 0}

    def when(conds, body):
        if not conds:
            body()
            return
        cond = conds[0]
        for other in conds[1:]:
            cond = jnp.logical_and(cond, other)
        pl.when(cond)(body)

    barrier = pltpu.get_barrier_semaphore()
    for hop in to:
        when([exists[hop]] if hop in exists else [],
             lambda hop=hop: pl.semaphore_signal(barrier, inc=1, device_id=to[hop], device_id_type=MESH))

    own = [
        pltpu.make_async_copy(tok, g.at[ep, tp], loc.at[0]),
        pltpu.make_async_copy(ids, idb.at[ep], loc.at[1]),
        pltpu.make_async_copy(rt, rbuf.at[tp], loc.at[2]),
    ]
    for cp in own:
        cp.start()
    shared_copies = [
        pltpu.make_async_copy(a, b, ssem.at[i]) for i, (a, b) in enumerate(((swg, sgb), (swu, sub), (swd, sdb)))
    ]

    def weights(j, buf):
        return [
            pltpu.make_async_copy(a.at[j], b.at[buf], wsem.at[i, buf])
            for i, (a, b) in enumerate(((wg, wgb), (wu, wub), (wd, wdb)))
        ]

    for cp in shared_copies + weights(0, 0) + weights(1, 1):
        cp.start()
    pl.semaphore_wait(barrier, 3 + jnp.where(exists["u"], 1, 0) + jnp.where(exists["d"], 1, 0))
    for cp in own:
        cp.wait()

    def place(k, off, core):
        zs, xx, yy = z - off[0], (x + off[1]) % 2, (y + off[2]) % 2
        e, t = zs * 2 + xx, yy * 2 + core
        if k == 0:
            return idb.at[e]
        if k == 1:
            return rbuf.at[t]
        _, start, n = plan.every[k]
        return g.at[e, t, pl.ds(start, n), :]

    def valid(off):
        if off[0] > 0:
            return [z >= off[0]]
        if off[0] < 0:
            return [z < nz + off[0]]
        return []

    def hop_copy(k, off, hop):
        ref = place(k, off, c)
        return pltpu.make_async_remote_copy(
            src_ref=ref, dst_ref=ref,
            send_sem=send.at[plan.sends[k, off, hop]],
            recv_sem=recv.at[plan.recvs[k, moved(off, hop)]],
            device_id=to[hop], device_id_type=MESH)

    def arrival(k, off):
        ref = place(k, off, c)
        return pltpu.make_async_remote_copy(
            src_ref=ref, dst_ref=ref, send_sem=send.at[0], recv_sem=recv.at[plan.recvs[k, off]],
            device_id=to["c"], device_id_type=MESH)

    def pair_copy(k, off, core):
        ref = place(k, off, core)
        i = plan.pair[k, off]
        return pltpu.make_async_remote_copy(
            src_ref=ref, dst_ref=ref, send_sem=psend.at[i], recv_sem=precv.at[i],
            device_id=to["c"], device_id_type=MESH)

    for k, off in plan.events:
        order = plan.every[k][0]

        def step(k=k, off=off, order=order):
            if off != (0, 0, 0):
                arrival(k, off).wait_recv()
            for hop in next_hops(order, off, nz):
                when([exists[hop]] if hop in exists else [], lambda: hop_copy(k, off, hop).start())
            if k != 0:
                pair_copy(k, off, c).start()

        when(valid(off), step)

    def finish(k, off):
        for hop in next_hops(plan.every[k][0], off, nz):
            when([exists[hop]] if hop in exists else [], lambda: hop_copy(k, off, hop).wait_send())
        if k != 0:
            pair_copy(k, off, 1 - c).wait_recv()
            pair_copy(k, off, c).wait_send()

    for k, off in plan.events:
        when(valid(off), lambda k=k, off=off: finish(k, off))

    slots = n_ep * here

    @pl.loop(0, n_ep)
    def _(s):
        total = jnp.zeros((rows, 1), F32)
        for t in range(n_tp):
            v = g[s, t].astype(F32)
            total = total + jnp.sum(v * v, axis=-1, keepdims=True)
        inv = lax.rsqrt(total / (n_tp * width) + 1e-6)
        logits = jnp.zeros((slots, rows), F32)
        for t in range(n_tp):
            v = g[s, t].astype(F32) * inv * gain[:, t * width:(t + 1) * width]
            v = v.astype(BF16)
            g[s, t] = v
            logits = logits + lax.dot_general(rbuf[t], v, (((1,), (1,)), ((), ())), preferred_element_type=F32)
        names = lax.broadcasted_iota(jnp.int32, (slots, rows), 0)
        logits = jnp.where(names < experts, logits, -1e30)
        ex = jnp.exp(logits - jnp.max(logits, axis=0, keepdims=True))
        ex = jnp.where(names < experts, ex, 0.0)
        pr[...] = ex / jnp.sum(ex, axis=0, keepdims=True)
        probs = pr[pl.ds(pl.multiple_of(ep * here, here), here), :]
        mine = ep * here + lax.broadcasted_iota(jnp.int32, (here, rows), 0)
        match = jnp.zeros((here, rows), jnp.bool_)
        for q in range(ids.shape[0]):
            match = jnp.logical_or(match, mine == idb[s, q:q + 1, :])
        hit = jnp.where(match, 1.0, 0.0)
        upper = jnp.where(
            lax.broadcasted_iota(jnp.int32, (rows, rows), 0) < lax.broadcasted_iota(jnp.int32, (rows, rows), 1), 1.0, 0.0)
        rank = jnp.dot(hit.astype(BF16), upper.astype(BF16), preferred_element_type=F32)
        spot = jnp.where(match, rank, -1.0).astype(jnp.int32)
        spots = lax.broadcasted_iota(jnp.int32, (cap, rows), 0)
        for j in range(here):
            one = spot[j:j + 1, :] == spots
            sw[j, pl.ds(pl.multiple_of(s * cap, cap), cap), :] = jnp.sum(
                jnp.where(one, probs[j:j + 1, :], 0.0), axis=1, keepdims=True)
            pick[s, j * cap:(j + 1) * cap, :] = jnp.where(one, 1.0, 0.0).astype(BF16)
        for t in range(n_tp):
            v = jnp.dot(pick[s], g[s, t], preferred_element_type=F32).astype(BF16)
            for j in range(here):
                xs[j, pl.ds(pl.multiple_of(s * cap, cap), cap), t * width:(t + 1) * width] = v[j * cap:(j + 1) * cap]

    for cp in shared_copies:
        cp.wait()
    sg = jnp.zeros((rows, sgb.shape[1]), F32)
    su = jnp.zeros((rows, sgb.shape[1]), F32)
    gate = jnp.zeros((rows, 1), F32)
    for t in range(n_tp):
        v = g[ep, t]
        sg = sg + jnp.dot(v, sgb[t * width:(t + 1) * width, :], preferred_element_type=F32)
        su = su + jnp.dot(v, sub[t * width:(t + 1) * width, :], preferred_element_type=F32)
        gate = gate + jnp.sum(v.astype(F32) * sgw[:, t * width:(t + 1) * width].astype(F32), axis=-1, keepdims=True)
    sh = (sg / (1.0 + jnp.exp(-sg)) * su).astype(BF16)
    gate = 1.0 / (1.0 + jnp.exp(-gate))
    for t in range(n_tp):
        part[t] = gate * jnp.dot(sh, sdb[:, t * width:(t + 1) * width], preferred_element_type=F32)

    @pl.loop(0, here)
    def _(j):
        buf = j % 2
        for cp in weights(j, buf):
            cp.wait()
        v = xs[j]
        a = jnp.dot(v, wgb[buf], preferred_element_type=F32)
        b = jnp.dot(v, wub[buf], preferred_element_type=F32)
        h = (a / (1.0 + jnp.exp(-a)) * b).astype(BF16)
        for t in range(n_tp):
            o = jnp.dot(h, wdb[buf, :, t * width:(t + 1) * width], preferred_element_type=F32)
            xs[j, :, t * width:(t + 1) * width] = (o * sw[j]).astype(BF16)

        @pl.when(j + 2 < here)
        def _():
            for cp in weights(j + 2, buf):
                cp.start()

    @pl.loop(0, n_ep)
    def _(s):
        for t in range(n_tp):
            v = xs[:, pl.ds(pl.multiple_of(s * cap, cap), cap), t * width:(t + 1) * width]
            v = v.reshape(here * cap, width)
            o = lax.dot_general(pick[s], v, (((0,), (0,)), ((), ())), preferred_element_type=F32)
            o = o + jnp.where(s == ep, part[t], 0.0)
            g[s, t] = o.astype(BF16)

    def pair_back(k, off, core):
        ref = place(k, off, core)
        zs, xx, yy = z - off[0], (x + off[1]) % 2, (y + off[2]) % 2
        _, start, n = plan.every[k]
        i = plan.parents[k, off]
        return pltpu.make_async_remote_copy(
            src_ref=ref, dst_ref=cbuf.at[zs * 2 + xx, yy, pl.ds(start, n), :],
            send_sem=bpsend.at[i], recv_sem=bprecv.at[i], device_id=to["c"], device_id_type=MESH)

    def child_copy(k, off, hop):
        i, start = plan.slots[k, off, hop]
        ref = slot.at[pl.ds(start, plan.every[k][2]), :]
        return pltpu.make_async_remote_copy(
            src_ref=ref, dst_ref=ref, send_sem=bsend.at[0], recv_sem=brecv.at[i],
            device_id=to["c"], device_id_type=MESH), ref

    def parent(k, off):
        order = plan.every[k][0]
        d = order[last_dim(order, off)]
        if d == "z":
            hop = "d" if off[0] > 0 else "u"
            seen = "u" if off[0] > 0 else "d"
        else:
            hop = seen = d
        up = moved(off, hop)
        i, start = plan.slots[k, up, seen]
        return pltpu.make_async_remote_copy(
            src_ref=place(k, off, c), dst_ref=slot.at[pl.ds(start, plan.every[k][2]), :],
            send_sem=bsend.at[plan.parents[k, off]], recv_sem=brecv.at[i],
            device_id=to[hop], device_id_type=MESH)

    for k, off in plan.back:
        when(valid(off), lambda k=k, off=off: pair_back(k, off, 1 - c).start())
    for k, off in plan.back:
        def step(k=k, off=off):
            _, start, n = plan.every[k]
            zs, xx, yy = z - off[0], (x + off[1]) % 2, (y + off[2]) % 2
            pair_back(k, off, c).wait_recv()
            mine = place(k, off, c)
            acc = mine[...].astype(F32) + cbuf[zs * 2 + xx, yy, start:start + n, :].astype(F32)
            for hop in next_hops(plan.every[k][0], off, nz):
                cp, ref = child_copy(k, off, hop)
                if hop in exists:
                    pl.when(exists[hop])(lambda cp=cp: cp.wait_recv())
                    acc = acc + jnp.where(exists[hop], ref[...].astype(F32), 0.0)
                else:
                    cp.wait_recv()
                    acc = acc + ref[...].astype(F32)
            if off == (0, 0, 0):
                out[start:start + n, :] = acc.astype(BF16)
            else:
                mine[...] = acc.astype(BF16)
                parent(k, off).start()
        when(valid(off), step)
    for k, off in plan.back:
        def done(k=k, off=off):
            pair_back(k, off, 1 - c).wait_send()
            if off != (0, 0, 0):
                parent(k, off).wait_send()
        when(valid(off), done)


def fused_plan(mesh, tokens, norm_gain, router_weight, shared_gate_w, expert_ids, w_gate, w_up, w_down,
               shared_w_gate, shared_w_up, shared_w_down):
    rows, width = tokens.shape
    n_ep, n_tp = mesh.shape["ep"], mesh.shape["tp"]
    here, full, hid = w_gate.shape
    experts = router_weight.shape[1]
    shid = shared_w_gate.shape[1]
    slots, cap = n_ep * here, rows // 8
    plan = Plan(n_ep, rows)
    rt = jnp.pad(router_weight.T, ((0, slots - experts), (0, 0)))
    ids = jnp.pad(expert_ids.T, ((0, -expert_ids.shape[1] % 8), (0, 0)), constant_values=-1)
    vmem, hbm = pl.BlockSpec(memory_space=pltpu.VMEM), pl.BlockSpec(memory_space=pl.ANY)
    dma = pltpu.SemaphoreType.DMA
    return pl.pallas_call(
        functools.partial(kernel, plan, n_tp, here, experts),
        out_shape=jax.ShapeDtypeStruct((rows, width), BF16),
        in_specs=[hbm, vmem, vmem, hbm, hbm] + [hbm] * 6,
        out_specs=vmem,
        scratch_shapes=[
            pltpu.VMEM((n_ep, n_tp, rows, width), BF16),
            pltpu.VMEM((here, n_ep * cap, full), BF16),
            pltpu.VMEM((n_ep, here * cap, rows), BF16),
            pltpu.VMEM((here, n_ep * cap, 1), F32),
            pltpu.VMEM((slots, rows), F32),
            pltpu.VMEM((n_tp, rows, width), F32),
            pltpu.VMEM((n_tp, slots, width), BF16),
            pltpu.VMEM((n_ep,) + ids.shape, jnp.int32),
            pltpu.VMEM((2, full, hid), BF16),
            pltpu.VMEM((2, full, hid), BF16),
            pltpu.VMEM((2, hid, full), BF16),
            pltpu.VMEM((full, shid), BF16),
            pltpu.VMEM((full, shid), BF16),
            pltpu.VMEM((shid, full), BF16),
            pltpu.VMEM((plan.slot_rows, width), BF16),
            pltpu.VMEM((n_ep, n_tp // 2, rows, width), BF16),
            dma((3,)), dma((3, 2)), dma((3,)),
            dma((len(plan.sends),)), dma((len(plan.recvs),)), dma((len(plan.pair),)), dma((len(plan.pair),)),
            dma((len(plan.back),)), dma((len(plan.slots),)), dma((len(plan.back),)), dma((len(plan.back),)),
        ],
        compiler_params=pltpu.CompilerParams(
            collective_id=0, has_side_effects=True, vmem_limit_bytes=67043328),
    )(tokens, norm_gain.reshape(1, full), shared_gate_w.reshape(1, full), rt, ids, w_gate, w_up, w_down,
      shared_w_gate, shared_w_up, shared_w_down)


def fits(mesh, tokens, norm_gain, router_weight, shared_gate_w, expert_ids, w_gate, *rest):
    rows, width = tokens.shape
    n_ep, n_tp = mesh.shape["ep"], mesh.shape["tp"]
    return (
        n_ep in (4, 8)
        and n_tp == 4
        and rows % 256 == 0
        and width % 128 == 0
        and w_gate.shape[0] % 8 == 0
        and rows * width <= 1 << 17
        and w_gate.shape[0] * w_gate.shape[1] * w_gate.shape[2] <= 6 << 20
        and rest[2].shape[0] * rest[2].shape[1] <= 3 << 19
    )


def send_back(summed):
    return lax.all_to_all(summed, "ep", split_axis=0, concat_axis=0, tiled=True)


def expert_rows(arrived, w_gate, w_up, w_down):
    gate_act = jnp.einsum("sekd,edf->sekf", arrived, w_gate, preferred_element_type=jnp.float32)
    up_act = jnp.einsum("sekd,edf->sekf", arrived, w_up, preferred_element_type=jnp.float32)
    hidden = (jax.nn.silu(gate_act) * up_act).astype(jnp.bfloat16)
    partial_out = jnp.einsum("sekf,efd->sekd", hidden, w_down, preferred_element_type=jnp.float32)
    summed = lax.psum_scatter(partial_out, "tp", scatter_dimension=3, tiled=True).astype(
        jnp.bfloat16
    )
    return send_back(summed)


def sliced_rows(arrived, w_gate, w_up, w_down):
    complete = lax.all_gather(arrived, "tp", axis=3, tiled=True)
    return expert_rows(complete, w_gate, w_up, w_down)


def dispatch_plan(
    tokens,
    norm_gain,
    router_weight,
    shared_gate_w,
    expert_ids,
    w_gate,
    w_up,
    w_down,
    shared_w_gate,
    shared_w_up,
    shared_w_down,
):
    width = tokens.shape[1]
    tok_rows = tokens.shape[0]
    column_start = lax.axis_index("tp") * width
    whole = lax.all_gather(tokens, "tp", axis=1, tiled=True)
    values = whole.astype(jnp.float32)
    inv_rms = lax.rsqrt(jnp.mean(values * values, axis=-1, keepdims=True) + 1e-06)
    normed = (values * inv_rms * norm_gain[None, :]).astype(jnp.bfloat16)
    own_part = lax.dynamic_slice_in_dim(normed, column_start, width, 1)
    partial_logits = jnp.dot(own_part, router_weight, preferred_element_type=jnp.float32)
    logits = lax.psum(partial_logits, "tp")
    probs = jax.nn.softmax(logits, axis=-1)
    expert_count = logits.shape[1]
    matches = expert_ids[:, :, None] == jnp.arange(expert_count, dtype=jnp.int32)[None, None, :]
    route_weight = jnp.sum(jnp.where(matches, probs[:, None, :], 0.0), axis=-1)
    gate_whole, up_whole, down_whole = (w_gate, w_up, w_down)
    experts_here = w_gate.shape[0]
    slot_count = lax.axis_size("ep") * experts_here
    capacity = tok_rows // 8
    flat_ids = expert_ids.reshape(-1)
    one_hot = (flat_ids[:, None] == jnp.arange(slot_count, dtype=jnp.int32)[None, :]).astype(
        jnp.int32
    )
    before = jnp.cumsum(one_hot, axis=0) - one_hot
    order_rank = jnp.sum(before * one_hot, axis=1)
    slot_ids = (flat_ids * capacity + order_rank).reshape(expert_ids.shape)
    targets = jnp.arange(slot_count * capacity, dtype=jnp.int32)
    dispatch_map = jnp.sum(
        (slot_ids[None, :, :] == targets[:, None, None]).astype(jnp.bfloat16), axis=2
    )
    outgoing = jnp.dot(dispatch_map, own_part, preferred_element_type=jnp.float32).astype(
        jnp.bfloat16
    )
    outgoing = outgoing.reshape(lax.axis_size("ep"), experts_here, capacity, width)
    returned = sliced_rows(
        lax.all_to_all(outgoing, "ep", split_axis=0, concat_axis=0, tiled=True),
        w_gate=gate_whole,
        w_up=up_whole,
        w_down=down_whole,
    )
    picked = returned.reshape(slot_count * capacity, width)[slot_ids]
    routed = jnp.sum(route_weight[:, :, None] * picked.astype(jnp.float32), axis=1)
    shared_gate_act = jnp.dot(normed, shared_w_gate, preferred_element_type=jnp.float32)
    shared_up_act = jnp.dot(normed, shared_w_up, preferred_element_type=jnp.float32)
    shared_hidden = (jax.nn.silu(shared_gate_act) * shared_up_act).astype(jnp.bfloat16)
    shared_part = jnp.dot(shared_hidden, shared_w_down, preferred_element_type=jnp.float32)
    shared_own = lax.psum_scatter(shared_part, "tp", scatter_dimension=1, tiled=True)
    share_gate = jax.nn.sigmoid(jnp.dot(normed, shared_gate_w, preferred_element_type=jnp.float32))
    return (share_gate[:, None] * shared_own + routed).astype(jnp.bfloat16)


def gather_plan(
    tokens,
    norm_gain,
    router_weight,
    shared_gate_w,
    expert_ids,
    w_gate,
    w_up,
    w_down,
    shared_w_gate,
    shared_w_up,
    shared_w_down,
):
    rows, width = tokens.shape
    n_ep = lax.axis_size("ep")
    n_tp = lax.axis_size("tp")
    full = n_tp * width
    here = w_gate.shape[0]
    cap = rows // 8
    me = lax.axis_index("ep")

    every = lax.all_gather(tokens, ("ep", "tp"), axis=0)
    ids = lax.all_gather(expert_ids.reshape(-1), "ep", axis=0)
    ids = ids.reshape(n_ep, rows, expert_ids.shape[1])
    router = lax.all_gather(router_weight, "tp", axis=0, tiled=True)

    whole = every.reshape(n_ep, n_tp, rows, width).transpose(0, 2, 1, 3)
    values = whole.reshape(n_ep, rows, full).astype(F32)
    inv_rms = lax.rsqrt(jnp.mean(values * values, axis=-1, keepdims=True) + 1e-06)
    normed = (values * inv_rms * norm_gain).astype(BF16)

    logits = jnp.einsum("std,dx->stx", normed, router, preferred_element_type=F32)
    probs = jax.nn.softmax(logits, axis=-1)
    probs = jnp.pad(probs, ((0, 0), (0, 0), (0, n_ep * here - probs.shape[-1])))
    local = lax.dynamic_slice_in_dim(probs, me * here, here, 2)
    names = me * here + jnp.arange(here, dtype=jnp.int32)
    match = jnp.any(ids[:, :, :, None] == names, axis=2)
    lower = jnp.tril(jnp.ones((rows, rows), BF16), -1)
    rank = jnp.einsum("tu,suj->sjt", lower, match.astype(BF16), preferred_element_type=F32)
    match_t = match.transpose(0, 2, 1)
    spot = jnp.where(match_t, rank, -1.0).astype(jnp.int32)
    pick = spot[:, :, None, :] == jnp.arange(cap, dtype=jnp.int32)[None, None, :, None]
    slot_w = jnp.sum(jnp.where(pick, local.transpose(0, 2, 1)[:, :, None, :], 0.0), axis=-1)
    pick = pick.astype(BF16)

    x = jnp.einsum("sjkt,std->jskd", pick, normed, preferred_element_type=F32).astype(BF16)
    gate = jnp.einsum("jskd,jdf->jskf", x, w_gate, preferred_element_type=F32)
    up = jnp.einsum("jskd,jdf->jskf", x, w_up, preferred_element_type=F32)
    hidden = (jax.nn.silu(gate) * up).astype(BF16)
    y = jnp.einsum("jskf,jfd->jskd", hidden, w_down, preferred_element_type=F32)
    y = (y * slot_w.transpose(1, 0, 2)[..., None]).astype(BF16)
    routed = jnp.einsum("sjkt,jskd->std", pick, y, preferred_element_type=F32)

    own = lax.dynamic_index_in_dim(normed, me, 0, keepdims=False)
    sg = jnp.dot(own, shared_w_gate, preferred_element_type=F32)
    su = jnp.dot(own, shared_w_up, preferred_element_type=F32)
    sh = (jax.nn.silu(sg) * su).astype(BF16)
    part = jnp.dot(sh, shared_w_down, preferred_element_type=F32)
    share = jax.nn.sigmoid(jnp.dot(own, shared_gate_w, preferred_element_type=F32))
    part = share[:, None] * part
    mine = (jnp.arange(n_ep) == me)[:, None, None]
    total = (routed + jnp.where(mine, part[None], 0.0)).astype(BF16)
    total = total.reshape(n_ep, rows, n_tp, width)
    total = lax.psum_scatter(total, "tp", scatter_dimension=2, tiled=True)
    total = total.reshape(n_ep * rows, width)
    terms = lax.all_to_all(total, "ep", split_axis=0, concat_axis=0, tiled=True)
    return jnp.sum(terms.reshape(n_ep, rows, width).astype(F32), axis=0).astype(BF16)


def solution(mesh):
    def per_device(tokens, *rest):
        gathered = mesh.size * tokens.size * tokens.dtype.itemsize
        if gathered <= 16 << 20 and fits(mesh, tokens, *rest):
            return fused_plan(mesh, tokens, *rest)
        plan = gather_plan if gathered <= 16 << 20 else dispatch_plan
        return plan(tokens, *rest)

    return jax.shard_map(
        per_device,
        mesh=mesh,
        in_specs=(
            P("ep", "tp"),
            P(),
            P("tp", None),
            P(),
            P("ep", None),
            P("ep", None, "tp"),
            P("ep", None, "tp"),
            P("ep", "tp", None),
            P(None, "tp"),
            P(None, "tp"),
            P("tp", None),
        ),
        out_specs=P("ep", "tp"),
        check_vma=False,
    )
```

```python
import functools

import jax
import jax.numpy as jnp
from jax import lax
from jax.experimental import pallas as pl
from jax.experimental.pallas import tpu as pltpu
from jax.sharding import PartitionSpec as P

F32 = jnp.float32
BF16 = jnp.bfloat16
MESH = pl.DeviceIdType.MESH


def offsets(nz, order):
    span = {"z": range(-(nz - 1), nz), "x": (0, 1), "y": (0, 1)}
    take = lambda d: span[d] if d in order else (0,)
    return [(a, b, c) for a in take("z") for b in take("x") for c in take("y")]


def last_dim(order, off):
    value = dict(zip("zxy", off))
    return max([i for i, d in enumerate(order) if value[d] != 0], default=-1)


def next_hops(order, off, nz):
    last, dz = last_dim(order, off), off[0]
    hops = []
    for i, d in enumerate(order):
        if d == "z":
            if (last < i or (last == i and dz > 0)) and dz < nz - 1:
                hops.append("u")
            if (last < i or (last == i and dz < 0)) and dz > 1 - nz:
                hops.append("d")
        elif last < i:
            hops.append(d)
    return hops


def moved(off, hop):
    dz, dx, dy = off
    return {
        "u": (dz + 1, dx, dy),
        "d": (dz - 1, dx, dy),
        "x": (dz, 1 - dx, dy),
        "y": (dz, dx, 1 - dy),
    }[hop]


def event_order(nz, streams):
    events = []
    for k, (order, _, n) in enumerate(streams):
        for off in offsets(nz, order):
            value = {"z": abs(off[0]), "x": off[1], "y": off[2]}
            when, load = 0.0, 1
            for d in order:
                when += value[d] * load * n
                load *= nz if d == "z" else 2
            events.append((when, k, off))
    events.sort()
    return [(k, off) for _, k, off in events]


def block_streams(rows):
    part = rows // 16
    cuts = (("zxy", 3 * part), ("zyx", 3 * part), ("xzy", 5 * part), ("yzx", 5 * part))
    streams, start = [], 0
    for order, n in cuts:
        streams.append((order, start, n))
        start += n
    return streams


class Plan:
    def __init__(self, n_ep, rows):
        self.nz = n_ep // 2
        self.streams = block_streams(rows)
        self.extra = [("zx", 0, 1), ("y", 0, 1)]
        every = self.extra + self.streams
        self.events = event_order(self.nz, every)
        self.sends, self.recvs, self.pair = {}, {}, {}
        for k, off in self.events:
            for hop in next_hops(every[k][0], off, self.nz):
                self.sends[k, off, hop] = len(self.sends)
            self.recvs[k, off] = len(self.recvs)
            if k != 0:
                self.pair[k, off] = len(self.pair)
        self.every = every
        self.back = [(k, off) for k, off in reversed(self.events) if k >= 2]
        self.slots, self.slot_rows = {}, 0
        for k, off in self.back:
            for hop in next_hops(every[k][0], off, self.nz):
                self.slots[k, off, hop] = (len(self.slots), self.slot_rows)
                self.slot_rows += every[k][2]
        self.parents = {e: i for i, e in enumerate(self.back)}


def kernel(plan, n_tp, here, experts,
           tok, gain, sgw, rt, ids, wg, wu, wd, swg, swu, swd, out,
           g, xs, pick, sw, pr, part, rbuf, idb, wab, wdb, sab, sdb, mine, slot, cbuf,
           loc, wsem, ssem, send, recv, psend, precv, bsend, brecv, bpsend, bprecv):
    nz = plan.nz
    ep, tp = lax.axis_index("ep"), lax.axis_index("tp")
    z, x, y, c = ep // 2, ep % 2, tp // 2, tp % 2
    rows, width = tok.shape
    n_ep = 2 * nz
    cap = rows // 8

    def dev(z_, x_, y_, c_):
        return (z_ * 2 + x_, y_ * 2 + c_)

    to = {
        "u": dev(z + 1, x, y, c),
        "d": dev(z - 1, x, y, c),
        "x": dev(z, 1 - x, y, c),
        "y": dev(z, x, 1 - y, c),
        "c": dev(z, x, y, 1 - c),
    }
    exists = {"u": z < nz - 1, "d": z > 0}

    def when(conds, body):
        if not conds:
            body()
            return
        cond = conds[0]
        for other in conds[1:]:
            cond = jnp.logical_and(cond, other)
        pl.when(cond)(body)

    barrier = pltpu.get_barrier_semaphore()
    for hop in to:
        when([exists[hop]] if hop in exists else [],
             lambda hop=hop: pl.semaphore_signal(barrier, inc=1, device_id=to[hop], device_id_type=MESH))

    own = [
        pltpu.make_async_copy(tok, g.at[ep, tp], loc.at[0]),
        pltpu.make_async_copy(ids, idb.at[ep], loc.at[1]),
        pltpu.make_async_copy(rt, rbuf.at[tp], loc.at[2]),
    ]
    for cp in own:
        cp.start()
    hid, shid = wg.shape[1], swg.shape[0]
    shared_copies = [
        pltpu.make_async_copy(swg, sab.at[0:shid], ssem.at[0]),
        pltpu.make_async_copy(swu, sab.at[shid:2 * shid], ssem.at[1]),
        pltpu.make_async_copy(swd, sdb, ssem.at[2]),
    ]

    def weights(j, buf):
        return [
            pltpu.make_async_copy(wg.at[j], wab.at[buf, 0:hid], wsem.at[0, buf]),
            pltpu.make_async_copy(wu.at[j], wab.at[buf, hid:2 * hid], wsem.at[1, buf]),
            pltpu.make_async_copy(wd.at[j], wdb.at[buf], wsem.at[2, buf]),
        ]

    for cp in shared_copies + weights(0, 0) + weights(1, 1):
        cp.start()
    pl.semaphore_wait(barrier, 3 + jnp.where(exists["u"], 1, 0) + jnp.where(exists["d"], 1, 0))
    for cp in own:
        cp.wait()

    def place(k, off, core):
        zs, xx, yy = z - off[0], (x + off[1]) % 2, (y + off[2]) % 2
        e, t = zs * 2 + xx, yy * 2 + core
        if k == 0:
            return idb.at[e]
        if k == 1:
            return rbuf.at[t]
        _, start, n = plan.every[k]
        return g.at[e, t, pl.ds(start, n), :]

    def valid(off):
        if off[0] > 0:
            return [z >= off[0]]
        if off[0] < 0:
            return [z < nz + off[0]]
        return []

    def hop_copy(k, off, hop):
        ref = place(k, off, c)
        return pltpu.make_async_remote_copy(
            src_ref=ref, dst_ref=ref,
            send_sem=send.at[plan.sends[k, off, hop]],
            recv_sem=recv.at[plan.recvs[k, moved(off, hop)]],
            device_id=to[hop], device_id_type=MESH)

    def arrival(k, off):
        ref = place(k, off, c)
        return pltpu.make_async_remote_copy(
            src_ref=ref, dst_ref=ref, send_sem=send.at[0], recv_sem=recv.at[plan.recvs[k, off]],
            device_id=to["c"], device_id_type=MESH)

    def pair_copy(k, off, core):
        ref = place(k, off, core)
        i = plan.pair[k, off]
        return pltpu.make_async_remote_copy(
            src_ref=ref, dst_ref=ref, send_sem=psend.at[i], recv_sem=precv.at[i],
            device_id=to["c"], device_id_type=MESH)

    for k, off in plan.events:
        order = plan.every[k][0]

        def step(k=k, off=off, order=order):
            if off != (0, 0, 0):
                arrival(k, off).wait_recv()
            for hop in next_hops(order, off, nz):
                when([exists[hop]] if hop in exists else [], lambda: hop_copy(k, off, hop).start())
            if k != 0:
                pair_copy(k, off, c).start()

        when(valid(off), step)

    def finish(k, off):
        for hop in next_hops(plan.every[k][0], off, nz):
            when([exists[hop]] if hop in exists else [], lambda: hop_copy(k, off, hop).wait_send())
        if k != 0:
            pair_copy(k, off, 1 - c).wait_recv()
            pair_copy(k, off, c).wait_send()

    for k, off in plan.events:
        when(valid(off), lambda k=k, off=off: finish(k, off))

    pr[...] = jnp.zeros_like(pr)

    @pl.loop(0, n_ep)
    def _(s):
        total = jnp.zeros((rows, 1), F32)
        for t in range(n_tp):
            v = g[s, t].astype(F32)
            total = total + jnp.sum(v * v, axis=-1, keepdims=True)
        inv = lax.rsqrt(total / (n_tp * width) + 1e-6)
        logits = jnp.zeros((experts, rows), F32)
        for t in range(n_tp):
            v = g[s, t].astype(F32) * inv * gain[:, t * width:(t + 1) * width]
            v = v.astype(BF16)
            g[s, t] = v
            logits = logits + lax.dot_general(rbuf[t], v, (((1,), (1,)), ((), ())), preferred_element_type=F32)
        ex = jnp.exp(logits - jnp.max(logits, axis=0, keepdims=True))
        pr[0:experts, :] = ex / jnp.sum(ex, axis=0, keepdims=True)
        probs = pr[pl.ds(pl.multiple_of(ep * here, here), here), :]
        names = ep * here + lax.broadcasted_iota(jnp.int32, (here, rows), 0)
        match = jnp.zeros((here, rows), jnp.bool_)
        for q in range(ids.shape[0]):
            match = jnp.logical_or(match, names == idb[s, q:q + 1, :])
        hit = jnp.where(match, 1.0, 0.0)
        upper = jnp.where(
            lax.broadcasted_iota(jnp.int32, (rows, rows), 0) < lax.broadcasted_iota(jnp.int32, (rows, rows), 1), 1.0, 0.0)
        rank = jnp.dot(hit.astype(BF16), upper.astype(BF16), preferred_element_type=F32)
        spot = jnp.where(match, rank, -1.0).astype(jnp.int32)
        spots = lax.broadcasted_iota(jnp.int32, (cap, rows), 0)
        for j in range(here):
            one = spot[j:j + 1, :] == spots
            sw[j, pl.ds(pl.multiple_of(s * cap, cap), cap), :] = jnp.sum(
                jnp.where(one, probs[j:j + 1, :], 0.0), axis=1, keepdims=True)
            pick[s, j * cap:(j + 1) * cap, :] = jnp.where(one, 1.0, 0.0).astype(BF16)
        for t in range(n_tp):
            v = jnp.dot(pick[s], g[s, t], preferred_element_type=F32).astype(BF16)
            for j in range(here):
                xs[j, pl.ds(pl.multiple_of(s * cap, cap), cap), t * width:(t + 1) * width] = v[j * cap:(j + 1) * cap]

    for cp in shared_copies:
        cp.wait()
    gate = jnp.zeros((rows, 1), F32)
    for t in range(n_tp):
        v = g[ep, t]
        mine[:, t * width:(t + 1) * width] = v
        gate = gate + jnp.sum(v.astype(F32) * sgw[:, t * width:(t + 1) * width].astype(F32), axis=-1, keepdims=True)
    ab = lax.dot_general(sab[...], mine[...], (((1,), (1,)), ((), ())), preferred_element_type=F32)
    a, b = ab[:shid], ab[shid:]
    h = (a / (1.0 + jnp.exp(-a)) * b).astype(BF16)
    gate = 1.0 / (1.0 + jnp.exp(-gate))
    for t in range(n_tp):
        part[t] = gate * lax.dot_general(
            h, sdb[:, t * width:(t + 1) * width], (((0,), (0,)), ((), ())), preferred_element_type=F32)

    @pl.loop(0, here)
    def _(j):
        buf = j % 2
        for cp in weights(j, buf):
            cp.wait()
        ab = lax.dot_general(wab[buf], xs[j], (((1,), (1,)), ((), ())), preferred_element_type=F32)
        a, b = ab[:hid], ab[hid:]
        h = (a / (1.0 + jnp.exp(-a)) * b).astype(BF16)
        for t in range(n_tp):
            o = lax.dot_general(
                h, wdb[buf, :, t * width:(t + 1) * width], (((0,), (0,)), ((), ())), preferred_element_type=F32)
            xs[j, :, t * width:(t + 1) * width] = (o * sw[j]).astype(BF16)

        @pl.when(j + 2 < here)
        def _():
            for cp in weights(j + 2, buf):
                cp.start()

    @pl.loop(0, n_ep)
    def _(s):
        for t in range(n_tp):
            v = xs[:, pl.ds(pl.multiple_of(s * cap, cap), cap), t * width:(t + 1) * width]
            v = v.reshape(here * cap, width)
            o = lax.dot_general(pick[s], v, (((0,), (0,)), ((), ())), preferred_element_type=F32)
            o = o + jnp.where(s == ep, part[t], 0.0)
            g[s, t] = o.astype(BF16)

    def pair_back(k, off, core):
        ref = place(k, off, core)
        zs, xx, yy = z - off[0], (x + off[1]) % 2, (y + off[2]) % 2
        _, start, n = plan.every[k]
        i = plan.parents[k, off]
        return pltpu.make_async_remote_copy(
            src_ref=ref, dst_ref=cbuf.at[zs * 2 + xx, yy, pl.ds(start, n), :],
            send_sem=bpsend.at[i], recv_sem=bprecv.at[i], device_id=to["c"], device_id_type=MESH)

    def child_copy(k, off, hop):
        i, start = plan.slots[k, off, hop]
        ref = slot.at[pl.ds(start, plan.every[k][2]), :]
        return pltpu.make_async_remote_copy(
            src_ref=ref, dst_ref=ref, send_sem=bsend.at[0], recv_sem=brecv.at[i],
            device_id=to["c"], device_id_type=MESH), ref

    def parent(k, off):
        order = plan.every[k][0]
        d = order[last_dim(order, off)]
        if d == "z":
            hop = "d" if off[0] > 0 else "u"
            seen = "u" if off[0] > 0 else "d"
        else:
            hop = seen = d
        up = moved(off, hop)
        i, start = plan.slots[k, up, seen]
        return pltpu.make_async_remote_copy(
            src_ref=place(k, off, c), dst_ref=slot.at[pl.ds(start, plan.every[k][2]), :],
            send_sem=bsend.at[plan.parents[k, off]], recv_sem=brecv.at[i],
            device_id=to[hop], device_id_type=MESH)

    for k, off in plan.back:
        when(valid(off), lambda k=k, off=off: pair_back(k, off, 1 - c).start())
    for k, off in plan.back:
        def step(k=k, off=off):
            _, start, n = plan.every[k]
            zs, xx, yy = z - off[0], (x + off[1]) % 2, (y + off[2]) % 2
            pair_back(k, off, c).wait_recv()
            held = place(k, off, c)
            acc = held[...].astype(F32) + cbuf[zs * 2 + xx, yy, start:start + n, :].astype(F32)
            for hop in next_hops(plan.every[k][0], off, nz):
                cp, ref = child_copy(k, off, hop)
                if hop in exists:
                    pl.when(exists[hop])(lambda cp=cp: cp.wait_recv())
                    acc = acc + jnp.where(exists[hop], ref[...].astype(F32), 0.0)
                else:
                    cp.wait_recv()
                    acc = acc + ref[...].astype(F32)
            if off == (0, 0, 0):
                out[start:start + n, :] = acc.astype(BF16)
            else:
                held[...] = acc.astype(BF16)
                parent(k, off).start()
        when(valid(off), step)
    for k, off in plan.back:
        def done(k=k, off=off):
            pair_back(k, off, 1 - c).wait_send()
            if off != (0, 0, 0):
                parent(k, off).wait_send()
        when(valid(off), done)


def fused_plan(mesh, tokens, norm_gain, router_weight, shared_gate_w, expert_ids, w_gate, w_up, w_down,
               shared_w_gate, shared_w_up, shared_w_down):
    rows, width = tokens.shape
    n_ep, n_tp = mesh.shape["ep"], mesh.shape["tp"]
    here, full, hid = w_gate.shape
    experts = router_weight.shape[1]
    shid = shared_w_gate.shape[1]
    slots, cap = n_ep * here, rows // 8
    plan = Plan(n_ep, rows)
    rt = router_weight.T
    ids = expert_ids.T
    vmem, hbm = pl.BlockSpec(memory_space=pltpu.VMEM), pl.BlockSpec(memory_space=pl.ANY)
    dma = pltpu.SemaphoreType.DMA
    return pl.pallas_call(
        functools.partial(kernel, plan, n_tp, here, experts),
        out_shape=jax.ShapeDtypeStruct((rows, width), BF16),
        in_specs=[hbm, vmem, vmem, hbm, hbm] + [hbm] * 6,
        out_specs=vmem,
        scratch_shapes=[
            pltpu.VMEM((n_ep, n_tp, rows, width), BF16),
            pltpu.VMEM((here, n_ep * cap, full), BF16),
            pltpu.VMEM((n_ep, here * cap, rows), BF16),
            pltpu.VMEM((here, n_ep * cap, 1), F32),
            pltpu.VMEM((slots, rows), F32),
            pltpu.VMEM((n_tp, rows, width), F32),
            pltpu.VMEM((n_tp, experts, width), BF16),
            pltpu.VMEM((n_ep,) + ids.shape, jnp.int32),
            pltpu.VMEM((2, 2 * hid, full), BF16),
            pltpu.VMEM((2, hid, full), BF16),
            pltpu.VMEM((2 * shid, full), BF16),
            pltpu.VMEM((shid, full), BF16),
            pltpu.VMEM((rows, full), BF16),
            pltpu.VMEM((plan.slot_rows, width), BF16),
            pltpu.VMEM((n_ep, n_tp // 2, rows, width), BF16),
            dma((3,)), dma((3, 2)), dma((3,)),
            dma((len(plan.sends),)), dma((len(plan.recvs),)), dma((len(plan.pair),)), dma((len(plan.pair),)),
            dma((len(plan.back),)), dma((len(plan.slots),)), dma((len(plan.back),)), dma((len(plan.back),)),
        ],
        compiler_params=pltpu.CompilerParams(
            collective_id=0, has_side_effects=True, vmem_limit_bytes=67043328),
    )(tokens, norm_gain.reshape(1, full), shared_gate_w.reshape(1, full), rt, ids,
      w_gate.transpose(0, 2, 1), w_up.transpose(0, 2, 1), w_down, shared_w_gate.T, shared_w_up.T, shared_w_down)


def fits(mesh, tokens, norm_gain, router_weight, shared_gate_w, expert_ids, w_gate, *rest):
    rows, width = tokens.shape
    n_ep, n_tp = mesh.shape["ep"], mesh.shape["tp"]
    return (
        n_ep in (4, 8)
        and n_tp == 4
        and rows % 256 == 0
        and width % 128 == 0
        and w_gate.shape[0] % 8 == 0
        and rows * width <= 1 << 17
        and w_gate.shape[0] * w_gate.shape[1] * w_gate.shape[2] <= 6 << 20
        and rest[2].shape[0] * rest[2].shape[1] <= 3 << 19
    )


def send_back(summed):
    return lax.all_to_all(summed, "ep", split_axis=0, concat_axis=0, tiled=True)


def expert_rows(arrived, w_gate, w_up, w_down):
    gate_act = jnp.einsum("sekd,edf->sekf", arrived, w_gate, preferred_element_type=jnp.float32)
    up_act = jnp.einsum("sekd,edf->sekf", arrived, w_up, preferred_element_type=jnp.float32)
    hidden = (jax.nn.silu(gate_act) * up_act).astype(jnp.bfloat16)
    partial_out = jnp.einsum("sekf,efd->sekd", hidden, w_down, preferred_element_type=jnp.float32)
    summed = lax.psum_scatter(partial_out, "tp", scatter_dimension=3, tiled=True).astype(
        jnp.bfloat16
    )
    return send_back(summed)


def sliced_rows(arrived, w_gate, w_up, w_down):
    complete = lax.all_gather(arrived, "tp", axis=3, tiled=True)
    return expert_rows(complete, w_gate, w_up, w_down)


def dispatch_plan(
    tokens,
    norm_gain,
    router_weight,
    shared_gate_w,
    expert_ids,
    w_gate,
    w_up,
    w_down,
    shared_w_gate,
    shared_w_up,
    shared_w_down,
):
    width = tokens.shape[1]
    tok_rows = tokens.shape[0]
    column_start = lax.axis_index("tp") * width
    whole = lax.all_gather(tokens, "tp", axis=1, tiled=True)
    values = whole.astype(jnp.float32)
    inv_rms = lax.rsqrt(jnp.mean(values * values, axis=-1, keepdims=True) + 1e-06)
    normed = (values * inv_rms * norm_gain[None, :]).astype(jnp.bfloat16)
    own_part = lax.dynamic_slice_in_dim(normed, column_start, width, 1)
    partial_logits = jnp.dot(own_part, router_weight, preferred_element_type=jnp.float32)
    logits = lax.psum(partial_logits, "tp")
    probs = jax.nn.softmax(logits, axis=-1)
    expert_count = logits.shape[1]
    matches = expert_ids[:, :, None] == jnp.arange(expert_count, dtype=jnp.int32)[None, None, :]
    route_weight = jnp.sum(jnp.where(matches, probs[:, None, :], 0.0), axis=-1)
    gate_whole, up_whole, down_whole = (w_gate, w_up, w_down)
    experts_here = w_gate.shape[0]
    slot_count = lax.axis_size("ep") * experts_here
    capacity = tok_rows // 8
    flat_ids = expert_ids.reshape(-1)
    one_hot = (flat_ids[:, None] == jnp.arange(slot_count, dtype=jnp.int32)[None, :]).astype(
        jnp.int32
    )
    before = jnp.cumsum(one_hot, axis=0) - one_hot
    order_rank = jnp.sum(before * one_hot, axis=1)
    slot_ids = (flat_ids * capacity + order_rank).reshape(expert_ids.shape)
    targets = jnp.arange(slot_count * capacity, dtype=jnp.int32)
    dispatch_map = jnp.sum(
        (slot_ids[None, :, :] == targets[:, None, None]).astype(jnp.bfloat16), axis=2
    )
    outgoing = jnp.dot(dispatch_map, own_part, preferred_element_type=jnp.float32).astype(
        jnp.bfloat16
    )
    outgoing = outgoing.reshape(lax.axis_size("ep"), experts_here, capacity, width)
    returned = sliced_rows(
        lax.all_to_all(outgoing, "ep", split_axis=0, concat_axis=0, tiled=True),
        w_gate=gate_whole,
        w_up=up_whole,
        w_down=down_whole,
    )
    picked = returned.reshape(slot_count * capacity, width)[slot_ids]
    routed = jnp.sum(route_weight[:, :, None] * picked.astype(jnp.float32), axis=1)
    shared_gate_act = jnp.dot(normed, shared_w_gate, preferred_element_type=jnp.float32)
    shared_up_act = jnp.dot(normed, shared_w_up, preferred_element_type=jnp.float32)
    shared_hidden = (jax.nn.silu(shared_gate_act) * shared_up_act).astype(jnp.bfloat16)
    shared_part = jnp.dot(shared_hidden, shared_w_down, preferred_element_type=jnp.float32)
    shared_own = lax.psum_scatter(shared_part, "tp", scatter_dimension=1, tiled=True)
    share_gate = jax.nn.sigmoid(jnp.dot(normed, shared_gate_w, preferred_element_type=jnp.float32))
    return (share_gate[:, None] * shared_own + routed).astype(jnp.bfloat16)


def gather_plan(
    tokens,
    norm_gain,
    router_weight,
    shared_gate_w,
    expert_ids,
    w_gate,
    w_up,
    w_down,
    shared_w_gate,
    shared_w_up,
    shared_w_down,
):
    rows, width = tokens.shape
    n_ep = lax.axis_size("ep")
    n_tp = lax.axis_size("tp")
    full = n_tp * width
    here = w_gate.shape[0]
    cap = rows // 8
    me = lax.axis_index("ep")

    every = lax.all_gather(tokens, ("ep", "tp"), axis=0)
    ids = lax.all_gather(expert_ids.reshape(-1), "ep", axis=0)
    ids = ids.reshape(n_ep, rows, expert_ids.shape[1])
    router = lax.all_gather(router_weight, "tp", axis=0, tiled=True)

    whole = every.reshape(n_ep, n_tp, rows, width).transpose(0, 2, 1, 3)
    values = whole.reshape(n_ep, rows, full).astype(F32)
    inv_rms = lax.rsqrt(jnp.mean(values * values, axis=-1, keepdims=True) + 1e-06)
    normed = (values * inv_rms * norm_gain).astype(BF16)

    logits = jnp.einsum("std,dx->stx", normed, router, preferred_element_type=F32)
    probs = jax.nn.softmax(logits, axis=-1)
    probs = jnp.pad(probs, ((0, 0), (0, 0), (0, n_ep * here - probs.shape[-1])))
    local = lax.dynamic_slice_in_dim(probs, me * here, here, 2)
    names = me * here + jnp.arange(here, dtype=jnp.int32)
    match = jnp.any(ids[:, :, :, None] == names, axis=2)
    lower = jnp.tril(jnp.ones((rows, rows), BF16), -1)
    rank = jnp.einsum("tu,suj->sjt", lower, match.astype(BF16), preferred_element_type=F32)
    match_t = match.transpose(0, 2, 1)
    spot = jnp.where(match_t, rank, -1.0).astype(jnp.int32)
    pick = spot[:, :, None, :] == jnp.arange(cap, dtype=jnp.int32)[None, None, :, None]
    slot_w = jnp.sum(jnp.where(pick, local.transpose(0, 2, 1)[:, :, None, :], 0.0), axis=-1)
    pick = pick.astype(BF16)

    x = jnp.einsum("sjkt,std->jskd", pick, normed, preferred_element_type=F32).astype(BF16)
    gate = jnp.einsum("jskd,jdf->jskf", x, w_gate, preferred_element_type=F32)
    up = jnp.einsum("jskd,jdf->jskf", x, w_up, preferred_element_type=F32)
    hidden = (jax.nn.silu(gate) * up).astype(BF16)
    y = jnp.einsum("jskf,jfd->jskd", hidden, w_down, preferred_element_type=F32)
    y = (y * slot_w.transpose(1, 0, 2)[..., None]).astype(BF16)
    routed = jnp.einsum("sjkt,jskd->std", pick, y, preferred_element_type=F32)

    own = lax.dynamic_index_in_dim(normed, me, 0, keepdims=False)
    sg = jnp.dot(own, shared_w_gate, preferred_element_type=F32)
    su = jnp.dot(own, shared_w_up, preferred_element_type=F32)
    sh = (jax.nn.silu(sg) * su).astype(BF16)
    part = jnp.dot(sh, shared_w_down, preferred_element_type=F32)
    share = jax.nn.sigmoid(jnp.dot(own, shared_gate_w, preferred_element_type=F32))
    part = share[:, None] * part
    mine = (jnp.arange(n_ep) == me)[:, None, None]
    total = (routed + jnp.where(mine, part[None], 0.0)).astype(BF16)
    total = total.reshape(n_ep, rows, n_tp, width)
    total = lax.psum_scatter(total, "tp", scatter_dimension=2, tiled=True)
    total = total.reshape(n_ep * rows, width)
    terms = lax.all_to_all(total, "ep", split_axis=0, concat_axis=0, tiled=True)
    return jnp.sum(terms.reshape(n_ep, rows, width).astype(F32), axis=0).astype(BF16)


def solution(mesh):
    def per_device(tokens, *rest):
        gathered = mesh.size * tokens.size * tokens.dtype.itemsize
        if gathered <= 16 << 20 and fits(mesh, tokens, *rest):
            return fused_plan(mesh, tokens, *rest)
        plan = gather_plan if gathered <= 16 << 20 else dispatch_plan
        return plan(tokens, *rest)

    return jax.shard_map(
        per_device,
        mesh=mesh,
        in_specs=(
            P("ep", "tp"),
            P(),
            P("tp", None),
            P(),
            P("ep", None),
            P("ep", None, "tp"),
            P("ep", None, "tp"),
            P("ep", "tp", None),
            P(None, "tp"),
            P(None, "tp"),
            P("tp", None),
        ),
        out_specs=P("ep", "tp"),
        check_vma=False,
    )
```

```python
import functools

import jax
import jax.numpy as jnp
from jax import lax
from jax.experimental import pallas as pl
from jax.experimental.pallas import tpu as pltpu
from jax.sharding import PartitionSpec as P

F32 = jnp.float32
BF16 = jnp.bfloat16
MESH = pl.DeviceIdType.MESH


def offsets(nz, order):
    span = {"z": range(-(nz - 1), nz), "x": (0, 1), "y": (0, 1)}
    take = lambda d: span[d] if d in order else (0,)
    return [(a, b, c) for a in take("z") for b in take("x") for c in take("y")]


def last_dim(order, off):
    value = dict(zip("zxy", off))
    return max([i for i, d in enumerate(order) if value[d] != 0], default=-1)


def next_hops(order, off, nz):
    last, dz = last_dim(order, off), off[0]
    hops = []
    for i, d in enumerate(order):
        if d == "z":
            if (last < i or (last == i and dz > 0)) and dz < nz - 1:
                hops.append("u")
            if (last < i or (last == i and dz < 0)) and dz > 1 - nz:
                hops.append("d")
        elif last < i:
            hops.append(d)
    return hops


def moved(off, hop):
    dz, dx, dy = off
    return {
        "u": (dz + 1, dx, dy),
        "d": (dz - 1, dx, dy),
        "x": (dz, 1 - dx, dy),
        "y": (dz, dx, 1 - dy),
    }[hop]


def event_order(nz, streams):
    events = []
    for k, (order, _, n) in enumerate(streams):
        for off in offsets(nz, order):
            value = {"z": abs(off[0]), "x": off[1], "y": off[2]}
            when, load = 0.0, 1
            for d in order:
                when += value[d] * load * n
                load *= nz if d == "z" else 2
            events.append((when, k, off))
    events.sort()
    return [(k, off) for _, k, off in events]


def block_streams(rows):
    part = rows // 16
    cuts = (("zxy", 3 * part), ("zyx", 3 * part), ("xzy", 5 * part), ("yzx", 5 * part))
    streams, start = [], 0
    for order, n in cuts:
        streams.append((order, start, n))
        start += n
    return streams


class Plan:
    def __init__(self, n_ep, rows):
        self.nz = n_ep // 2
        self.streams = block_streams(rows)
        self.extra = [("zx", 0, 1), ("y", 0, 1)]
        every = self.extra + self.streams
        self.events = event_order(self.nz, every)
        self.sends, self.recvs, self.pair = {}, {}, {}
        for k, off in self.events:
            for hop in next_hops(every[k][0], off, self.nz):
                self.sends[k, off, hop] = len(self.sends)
            self.recvs[k, off] = len(self.recvs)
            if k != 0:
                self.pair[k, off] = len(self.pair)
        self.every = every
        self.back = [(k, off) for k, off in reversed(self.events) if k >= 2]
        self.slots, self.slot_rows = {}, 0
        for k, off in self.back:
            for hop in next_hops(every[k][0], off, self.nz):
                self.slots[k, off, hop] = (len(self.slots), self.slot_rows)
                self.slot_rows += every[k][2]
        self.parents = {e: i for i, e in enumerate(self.back)}


def kernel(plan, n_tp, here, experts,
           tok, gain, sgw, rt, ids, wg, wu, wd, swg, swu, swd, out,
           g, xs, pick, sw, pr, part, rbuf, idb, wab, wdb, mine, nrm, hs, hb, ys, slot, cbuf,
           loc, wsem, ssem, send, recv, psend, precv, bsend, brecv, bpsend, bprecv):
    nz = plan.nz
    ep, tp = lax.axis_index("ep"), lax.axis_index("tp")
    z, x, y, c = ep // 2, ep % 2, tp // 2, tp % 2
    rows, width = tok.shape
    n_ep = 2 * nz
    cap = rows // 8

    def dev(z_, x_, y_, c_):
        return (z_ * 2 + x_, y_ * 2 + c_)

    to = {
        "u": dev(z + 1, x, y, c),
        "d": dev(z - 1, x, y, c),
        "x": dev(z, 1 - x, y, c),
        "y": dev(z, x, 1 - y, c),
        "c": dev(z, x, y, 1 - c),
    }
    exists = {"u": z < nz - 1, "d": z > 0}

    def when(conds, body):
        if not conds:
            body()
            return
        cond = conds[0]
        for other in conds[1:]:
            cond = jnp.logical_and(cond, other)
        pl.when(cond)(body)

    barrier = pltpu.get_barrier_semaphore()
    for hop in to:
        when([exists[hop]] if hop in exists else [],
             lambda hop=hop: pl.semaphore_signal(barrier, inc=1, device_id=to[hop], device_id_type=MESH))

    own = [
        pltpu.make_async_copy(tok, g.at[ep, tp], loc.at[0]),
        pltpu.make_async_copy(ids, idb.at[ep], loc.at[1]),
        pltpu.make_async_copy(rt, rbuf.at[tp], loc.at[2]),
    ]
    for cp in own:
        cp.start()
    hid, shid = wg.shape[1], swg.shape[0]
    deep = wab.shape[0] // (2 * hid)
    top, low = 4 * hid, 2 * hid
    shared_copies = [
        pltpu.make_async_copy(swg, wab.at[top:top + shid], ssem.at[0]),
        pltpu.make_async_copy(swu, wab.at[top + shid:top + 2 * shid], ssem.at[1]),
        pltpu.make_async_copy(swd, wdb.at[low:low + shid], ssem.at[2]),
    ]

    def rows_of(buf, n):
        return pl.ds(buf * n if isinstance(buf, int) else pl.multiple_of(buf * n, 16), n)

    def weights(j, buf):
        first, second = buf * (2 * hid), buf * (2 * hid) + hid
        if not isinstance(buf, int):
            first, second = pl.multiple_of(first, 16), pl.multiple_of(second, 16)
        return [
            pltpu.make_async_copy(wg.at[j], wab.at[pl.ds(first, hid)], wsem.at[0, buf]),
            pltpu.make_async_copy(wu.at[j], wab.at[pl.ds(second, hid)], wsem.at[1, buf]),
            pltpu.make_async_copy(wd.at[j], wdb.at[rows_of(buf, hid)], wsem.at[2, buf]),
        ]

    for cp in shared_copies + weights(0, 0) + weights(1, 1):
        cp.start()
    pl.semaphore_wait(barrier, 3 + jnp.where(exists["u"], 1, 0) + jnp.where(exists["d"], 1, 0))
    for cp in own:
        cp.wait()

    def place(k, off, core):
        zs, xx, yy = z - off[0], (x + off[1]) % 2, (y + off[2]) % 2
        e, t = zs * 2 + xx, yy * 2 + core
        if k == 0:
            return idb.at[e]
        if k == 1:
            return rbuf.at[t]
        _, start, n = plan.every[k]
        return g.at[e, t, pl.ds(start, n), :]

    def valid(off):
        if off[0] > 0:
            return [z >= off[0]]
        if off[0] < 0:
            return [z < nz + off[0]]
        return []

    def hop_copy(k, off, hop):
        ref = place(k, off, c)
        return pltpu.make_async_remote_copy(
            src_ref=ref, dst_ref=ref,
            send_sem=send.at[plan.sends[k, off, hop]],
            recv_sem=recv.at[plan.recvs[k, moved(off, hop)]],
            device_id=to[hop], device_id_type=MESH)

    def arrival(k, off):
        ref = place(k, off, c)
        return pltpu.make_async_remote_copy(
            src_ref=ref, dst_ref=ref, send_sem=send.at[0], recv_sem=recv.at[plan.recvs[k, off]],
            device_id=to["c"], device_id_type=MESH)

    def pair_copy(k, off, core):
        ref = place(k, off, core)
        i = plan.pair[k, off]
        return pltpu.make_async_remote_copy(
            src_ref=ref, dst_ref=ref, send_sem=psend.at[i], recv_sem=precv.at[i],
            device_id=to["c"], device_id_type=MESH)

    near = [sorted(range(nz), key=lambda v, p=p: abs(v - p)) for p in range(nz)]

    def ranked(rank):
        value = near[nz - 1][rank]
        for p in range(nz - 1):
            value = jnp.where(z == p, near[p][rank], value)
        return value

    def forward(k, off):
        order = plan.every[k][0]

        def step():
            if off != (0, 0, 0):
                arrival(k, off).wait_recv()
            for hop in next_hops(order, off, nz):
                when([exists[hop]] if hop in exists else [], lambda: hop_copy(k, off, hop).start())
            if k != 0:
                pair_copy(k, off, c).start()

        when(valid(off), step)

    pr[...] = jnp.zeros_like(pr)

    def source(rank, dx):
        for k, off in plan.events:
            if (k >= 2 and abs(off[0]) == rank and off[1] == dx) or (k == 1 and rank == 0 and dx == 0):
                when(valid(off), lambda k=k, off=off: pair_copy(k, off, 1 - c).wait_recv())
        s = ranked(rank) * 2 + (x + dx) % 2
        normed = mine if (rank, dx) == (0, 0) else nrm
        total = jnp.zeros((rows, 1), F32)
        for t in range(n_tp):
            v = g[s, t].astype(F32)
            total = total + jnp.sum(v * v, axis=-1, keepdims=True)
        inv = lax.rsqrt(total / (n_tp * width) + 1e-6)
        logits = jnp.zeros((experts, rows), F32)
        for t in range(n_tp):
            cols = slice(t * width, (t + 1) * width)
            v = (g[s, t].astype(F32) * inv * gain[:, cols]).astype(BF16)
            normed[:, cols] = v
            logits = logits + lax.dot_general(rbuf[t], v, (((1,), (1,)), ((), ())), preferred_element_type=F32)
        ex = jnp.exp(logits - jnp.max(logits, axis=0, keepdims=True))
        pr[0:experts, :] = ex / jnp.sum(ex, axis=0, keepdims=True)
        probs = pr[pl.ds(pl.multiple_of(ep * here, here), here), :]
        names = ep * here + lax.broadcasted_iota(jnp.int32, (here, rows), 0)
        match = jnp.zeros((here, rows), jnp.bool_)
        for q in range(ids.shape[0]):
            match = jnp.logical_or(match, names == idb[s, q:q + 1, :])
        hit = jnp.where(match, 1.0, 0.0)
        upper = jnp.where(
            lax.broadcasted_iota(jnp.int32, (rows, rows), 0) < lax.broadcasted_iota(jnp.int32, (rows, rows), 1), 1.0, 0.0)
        order_rank = jnp.dot(hit.astype(BF16), upper.astype(BF16), preferred_element_type=F32)
        spot = jnp.where(match, order_rank, -1.0).astype(jnp.int32)
        spots = lax.broadcasted_iota(jnp.int32, (cap, rows), 0)
        span = pl.ds(pl.multiple_of(s * cap, cap), cap)
        for j in range(here):
            one = spot[j:j + 1, :] == spots
            sw[j, span, :] = jnp.sum(jnp.where(one, probs[j:j + 1, :], 0.0), axis=1, keepdims=True)
            pick[s, j * cap:(j + 1) * cap, :] = jnp.where(one, 1.0, 0.0).astype(BF16)
        for t in range(n_tp):
            cols = slice(t * width, (t + 1) * width)
            v = jnp.dot(pick[s], normed[:, cols], preferred_element_type=F32).astype(BF16)
            for j in range(here):
                xs[j, span, cols] = v[j * cap:(j + 1) * cap]

    def shared_hidden():
        for cp in shared_copies:
            cp.wait()
        ab = lax.dot_general(
            wab[top:top + 2 * shid], mine[...], (((1,), (1,)), ((), ())), preferred_element_type=F32)
        a, b = ab[:shid], ab[shid:]
        hs[...] = (a / (1.0 + jnp.exp(-a)) * b).astype(BF16)

    def shared_out():
        gate = jnp.zeros((rows, 1), F32)
        for t in range(n_tp):
            cols = slice(t * width, (t + 1) * width)
            gate = gate + jnp.sum(
                mine[:, cols].astype(F32) * sgw[:, cols].astype(F32), axis=-1, keepdims=True)
        gate = 1.0 / (1.0 + jnp.exp(-gate))
        for t in range(n_tp):
            cols = slice(t * width, (t + 1) * width)
            part[t] = gate * lax.dot_general(
                hs[...], wdb[low:low + shid, cols], (((0,), (0,)), ((), ())), preferred_element_type=F32)
        for j in range(2, min(deep, here)):
            for cp in weights(j, j):
                cp.start()

    last = {}
    for i, (k, off) in enumerate(plan.events):
        rank, dx = abs(off[0]), off[1]
        for r in range(rank, nz):
            if k >= 2:
                last[r, dx] = i
            else:
                for both in (0, 1):
                    last[r, both] = i
    points = sorted(last, key=lambda r: (last[r], r))
    pieces = []
    for r in points:
        pieces.append((last[r] + 1000, functools.partial(source, *r)))
        if r == (0, 0):
            pieces.append((last[r] + 8, shared_hidden))
            pieces.append((last[r] + 12, shared_out))
    for i, (k, off) in enumerate(plan.events):
        forward(k, off)
        if pieces and pieces[0][0] <= i:
            pieces.pop(0)[1]()
    for _, piece in pieces:
        piece()

    def finish(k, off):
        for hop in next_hops(plan.every[k][0], off, nz):
            when([exists[hop]] if hop in exists else [], lambda: hop_copy(k, off, hop).wait_send())
        if k != 0:
            pair_copy(k, off, c).wait_send()

    for k, off in plan.events:
        when(valid(off), lambda k=k, off=off: finish(k, off))

    def hidden(j):
        ab = lax.dot_general(
            wab[rows_of(j % deep, 2 * hid)], xs[j], (((1,), (1,)), ((), ())), preferred_element_type=F32)
        a, b = ab[:hid], ab[hid:]
        return (a / (1.0 + jnp.exp(-a)) * b).astype(BF16)

    def down(j, h):
        for t in range(n_tp):
            cols = slice(t * width, (t + 1) * width)
            o = lax.dot_general(
                h, wdb[rows_of(j % deep, hid), cols], (((0,), (0,)), ((), ())), preferred_element_type=F32)
            ys[j, :, cols] = (o * sw[j]).astype(BF16)

    for cp in weights(0, 0):
        cp.wait()
    hb[...] = hidden(0)

    @pl.loop(1, here)
    def _(j):
        for cp in weights(j, j % deep):
            cp.wait()
        before = hb[...]
        hb[...] = hidden(j)
        down(j - 1, before)

        @pl.when(j - 1 + deep < here)
        def _():
            for cp in weights(j - 1 + deep, (j - 1) % deep):
                cp.start()

    down(here - 1, hb[...])

    def pair_back(k, off, core):
        ref = place(k, off, core)
        zs, xx, yy = z - off[0], (x + off[1]) % 2, (y + off[2]) % 2
        _, start, n = plan.every[k]
        i = plan.parents[k, off]
        return pltpu.make_async_remote_copy(
            src_ref=ref, dst_ref=cbuf.at[zs * 2 + xx, yy, pl.ds(start, n), :],
            send_sem=bpsend.at[i], recv_sem=bprecv.at[i], device_id=to["c"], device_id_type=MESH)

    def child_copy(k, off, hop):
        i, start = plan.slots[k, off, hop]
        ref = slot.at[pl.ds(start, plan.every[k][2]), :]
        return pltpu.make_async_remote_copy(
            src_ref=ref, dst_ref=ref, send_sem=bsend.at[0], recv_sem=brecv.at[i],
            device_id=to["c"], device_id_type=MESH), ref

    def parent(k, off):
        order = plan.every[k][0]
        d = order[last_dim(order, off)]
        if d == "z":
            hop = "d" if off[0] > 0 else "u"
            seen = "u" if off[0] > 0 else "d"
        else:
            hop = seen = d
        up = moved(off, hop)
        i, start = plan.slots[k, up, seen]
        return pltpu.make_async_remote_copy(
            src_ref=place(k, off, c), dst_ref=slot.at[pl.ds(start, plan.every[k][2]), :],
            send_sem=bsend.at[plan.parents[k, off]], recv_sem=brecv.at[i],
            device_id=to[hop], device_id_type=MESH)

    def tokens_of(rank, dx):
        s = ranked(nz - 1 - rank) * 2 + (x + dx) % 2
        span = pl.ds(pl.multiple_of(s * cap, cap), cap)
        for t in range(n_tp):
            v = ys[:, span, t * width:(t + 1) * width].reshape(here * cap, width)
            o = lax.dot_general(pick[s], v, (((0,), (0,)), ((), ())), preferred_element_type=F32)
            if rank == nz - 1 and dx == 0:
                o = o + part[t]
            g[s, t] = o.astype(BF16)
        for k, off in plan.back:
            if abs(off[0]) == nz - 1 - rank and off[1] == dx:
                when(valid(off), lambda k=k, off=off: pair_back(k, off, 1 - c).start())

    todo = [(rank, dx) for rank in range(nz) for dx in (1, 0)]
    for i, (k, off) in enumerate(plan.back):
        while todo and (i % 3 == 0 or (nz - 1 - abs(off[0]), off[1]) in todo):
            tokens_of(*todo.pop(0))
            if (nz - 1 - abs(off[0]), off[1]) not in todo:
                break

        def step(k=k, off=off):
            _, start, n = plan.every[k]
            zs, xx, yy = z - off[0], (x + off[1]) % 2, (y + off[2]) % 2
            pair_back(k, off, c).wait_recv()
            held = place(k, off, c)
            acc = held[...].astype(F32) + cbuf[zs * 2 + xx, yy, start:start + n, :].astype(F32)
            for hop in next_hops(plan.every[k][0], off, nz):
                cp, ref = child_copy(k, off, hop)
                if hop in exists:
                    pl.when(exists[hop])(lambda cp=cp: cp.wait_recv())
                    acc = acc + jnp.where(exists[hop], ref[...].astype(F32), 0.0)
                else:
                    cp.wait_recv()
                    acc = acc + ref[...].astype(F32)
            if off == (0, 0, 0):
                out[start:start + n, :] = acc.astype(BF16)
            else:
                held[...] = acc.astype(BF16)
                parent(k, off).start()
        when(valid(off), step)
    for k, off in plan.back:
        def done(k=k, off=off):
            pair_back(k, off, 1 - c).wait_send()
            if off != (0, 0, 0):
                parent(k, off).wait_send()
        when(valid(off), done)


def fused_plan(mesh, tokens, norm_gain, router_weight, shared_gate_w, expert_ids, w_gate, w_up, w_down,
               shared_w_gate, shared_w_up, shared_w_down):
    rows, width = tokens.shape
    n_ep, n_tp = mesh.shape["ep"], mesh.shape["tp"]
    here, full, hid = w_gate.shape
    experts = router_weight.shape[1]
    shid = shared_w_gate.shape[1]
    slots, cap = n_ep * here, rows // 8
    plan = Plan(n_ep, rows)
    rt = router_weight.T
    ids = expert_ids.T
    vmem, hbm = pl.BlockSpec(memory_space=pltpu.VMEM), pl.BlockSpec(memory_space=pl.ANY)
    dma = pltpu.SemaphoreType.DMA
    return pl.pallas_call(
        functools.partial(kernel, plan, n_tp, here, experts),
        out_shape=jax.ShapeDtypeStruct((rows, width), BF16),
        in_specs=[hbm, vmem, vmem, hbm, hbm] + [hbm] * 6,
        out_specs=vmem,
        scratch_shapes=[
            pltpu.VMEM((n_ep, n_tp, rows, width), BF16),
            pltpu.VMEM((here, n_ep * cap, full), BF16),
            pltpu.VMEM((n_ep, here * cap, rows), BF16),
            pltpu.VMEM((here, n_ep * cap, 1), F32),
            pltpu.VMEM((slots, rows), F32),
            pltpu.VMEM((n_tp, rows, width), F32),
            pltpu.VMEM((n_tp, experts, width), BF16),
            pltpu.VMEM((n_ep,) + ids.shape, jnp.int32),
            pltpu.VMEM((8 * hid, full), BF16),
            pltpu.VMEM((4 * hid, full), BF16),
            pltpu.VMEM((rows, full), BF16),
            pltpu.VMEM((rows, full), BF16),
            pltpu.VMEM((shid, rows), BF16),
            pltpu.VMEM((hid, n_ep * cap), BF16),
            pltpu.VMEM((here, n_ep * cap, full), BF16),
            pltpu.VMEM((plan.slot_rows, width), BF16),
            pltpu.VMEM((n_ep, n_tp // 2, rows, width), BF16),
            dma((3,)), dma((3, 4)), dma((3,)),
            dma((len(plan.sends),)), dma((len(plan.recvs),)), dma((len(plan.pair),)), dma((len(plan.pair),)),
            dma((len(plan.back),)), dma((len(plan.slots),)), dma((len(plan.back),)), dma((len(plan.back),)),
        ],
        compiler_params=pltpu.CompilerParams(
            collective_id=0, has_side_effects=True, vmem_limit_bytes=67043328),
    )(tokens, norm_gain.reshape(1, full), shared_gate_w.reshape(1, full), rt, ids,
      w_gate.transpose(0, 2, 1), w_up.transpose(0, 2, 1), w_down, shared_w_gate.T, shared_w_up.T, shared_w_down)


def fits(mesh, tokens, norm_gain, router_weight, shared_gate_w, expert_ids, w_gate, *rest):
    rows, width = tokens.shape
    n_ep, n_tp = mesh.shape["ep"], mesh.shape["tp"]
    return (
        n_ep in (4, 8)
        and n_tp == 4
        and rows % 256 == 0
        and width % 128 == 0
        and w_gate.shape[0] % 8 == 0
        and rows * width <= 1 << 17
        and w_gate.shape[0] * w_gate.shape[1] * w_gate.shape[2] <= 6 << 20
        and rest[2].shape[1] <= 2 * w_gate.shape[2]
        and w_gate.shape[2] % 16 == 0
        and w_gate.shape[0] >= 4
    )


def send_back(summed):
    return lax.all_to_all(summed, "ep", split_axis=0, concat_axis=0, tiled=True)


def expert_rows(arrived, w_gate, w_up, w_down):
    gate_act = jnp.einsum("sekd,edf->sekf", arrived, w_gate, preferred_element_type=jnp.float32)
    up_act = jnp.einsum("sekd,edf->sekf", arrived, w_up, preferred_element_type=jnp.float32)
    hidden = (jax.nn.silu(gate_act) * up_act).astype(jnp.bfloat16)
    partial_out = jnp.einsum("sekf,efd->sekd", hidden, w_down, preferred_element_type=jnp.float32)
    summed = lax.psum_scatter(partial_out, "tp", scatter_dimension=3, tiled=True).astype(
        jnp.bfloat16
    )
    return send_back(summed)


def sliced_rows(arrived, w_gate, w_up, w_down):
    complete = lax.all_gather(arrived, "tp", axis=3, tiled=True)
    return expert_rows(complete, w_gate, w_up, w_down)


def dispatch_plan(
    tokens,
    norm_gain,
    router_weight,
    shared_gate_w,
    expert_ids,
    w_gate,
    w_up,
    w_down,
    shared_w_gate,
    shared_w_up,
    shared_w_down,
):
    width = tokens.shape[1]
    tok_rows = tokens.shape[0]
    column_start = lax.axis_index("tp") * width
    whole = lax.all_gather(tokens, "tp", axis=1, tiled=True)
    values = whole.astype(jnp.float32)
    inv_rms = lax.rsqrt(jnp.mean(values * values, axis=-1, keepdims=True) + 1e-06)
    normed = (values * inv_rms * norm_gain[None, :]).astype(jnp.bfloat16)
    own_part = lax.dynamic_slice_in_dim(normed, column_start, width, 1)
    partial_logits = jnp.dot(own_part, router_weight, preferred_element_type=jnp.float32)
    logits = lax.psum(partial_logits, "tp")
    probs = jax.nn.softmax(logits, axis=-1)
    expert_count = logits.shape[1]
    matches = expert_ids[:, :, None] == jnp.arange(expert_count, dtype=jnp.int32)[None, None, :]
    route_weight = jnp.sum(jnp.where(matches, probs[:, None, :], 0.0), axis=-1)
    gate_whole, up_whole, down_whole = (w_gate, w_up, w_down)
    experts_here = w_gate.shape[0]
    slot_count = lax.axis_size("ep") * experts_here
    capacity = tok_rows // 8
    flat_ids = expert_ids.reshape(-1)
    one_hot = (flat_ids[:, None] == jnp.arange(slot_count, dtype=jnp.int32)[None, :]).astype(
        jnp.int32
    )
    before = jnp.cumsum(one_hot, axis=0) - one_hot
    order_rank = jnp.sum(before * one_hot, axis=1)
    slot_ids = (flat_ids * capacity + order_rank).reshape(expert_ids.shape)
    targets = jnp.arange(slot_count * capacity, dtype=jnp.int32)
    dispatch_map = jnp.sum(
        (slot_ids[None, :, :] == targets[:, None, None]).astype(jnp.bfloat16), axis=2
    )
    outgoing = jnp.dot(dispatch_map, own_part, preferred_element_type=jnp.float32).astype(
        jnp.bfloat16
    )
    outgoing = outgoing.reshape(lax.axis_size("ep"), experts_here, capacity, width)
    returned = sliced_rows(
        lax.all_to_all(outgoing, "ep", split_axis=0, concat_axis=0, tiled=True),
        w_gate=gate_whole,
        w_up=up_whole,
        w_down=down_whole,
    )
    picked = returned.reshape(slot_count * capacity, width)[slot_ids]
    routed = jnp.sum(route_weight[:, :, None] * picked.astype(jnp.float32), axis=1)
    shared_gate_act = jnp.dot(normed, shared_w_gate, preferred_element_type=jnp.float32)
    shared_up_act = jnp.dot(normed, shared_w_up, preferred_element_type=jnp.float32)
    shared_hidden = (jax.nn.silu(shared_gate_act) * shared_up_act).astype(jnp.bfloat16)
    shared_part = jnp.dot(shared_hidden, shared_w_down, preferred_element_type=jnp.float32)
    shared_own = lax.psum_scatter(shared_part, "tp", scatter_dimension=1, tiled=True)
    share_gate = jax.nn.sigmoid(jnp.dot(normed, shared_gate_w, preferred_element_type=jnp.float32))
    return (share_gate[:, None] * shared_own + routed).astype(jnp.bfloat16)


def gather_plan(
    tokens,
    norm_gain,
    router_weight,
    shared_gate_w,
    expert_ids,
    w_gate,
    w_up,
    w_down,
    shared_w_gate,
    shared_w_up,
    shared_w_down,
):
    rows, width = tokens.shape
    n_ep = lax.axis_size("ep")
    n_tp = lax.axis_size("tp")
    full = n_tp * width
    here = w_gate.shape[0]
    cap = rows // 8
    me = lax.axis_index("ep")

    every = lax.all_gather(tokens, ("ep", "tp"), axis=0)
    ids = lax.all_gather(expert_ids.reshape(-1), "ep", axis=0)
    ids = ids.reshape(n_ep, rows, expert_ids.shape[1])
    router = lax.all_gather(router_weight, "tp", axis=0, tiled=True)

    whole = every.reshape(n_ep, n_tp, rows, width).transpose(0, 2, 1, 3)
    values = whole.reshape(n_ep, rows, full).astype(F32)
    inv_rms = lax.rsqrt(jnp.mean(values * values, axis=-1, keepdims=True) + 1e-06)
    normed = (values * inv_rms * norm_gain).astype(BF16)

    logits = jnp.einsum("std,dx->stx", normed, router, preferred_element_type=F32)
    probs = jax.nn.softmax(logits, axis=-1)
    probs = jnp.pad(probs, ((0, 0), (0, 0), (0, n_ep * here - probs.shape[-1])))
    local = lax.dynamic_slice_in_dim(probs, me * here, here, 2)
    names = me * here + jnp.arange(here, dtype=jnp.int32)
    match = jnp.any(ids[:, :, :, None] == names, axis=2)
    lower = jnp.tril(jnp.ones((rows, rows), BF16), -1)
    rank = jnp.einsum("tu,suj->sjt", lower, match.astype(BF16), preferred_element_type=F32)
    match_t = match.transpose(0, 2, 1)
    spot = jnp.where(match_t, rank, -1.0).astype(jnp.int32)
    pick = spot[:, :, None, :] == jnp.arange(cap, dtype=jnp.int32)[None, None, :, None]
    slot_w = jnp.sum(jnp.where(pick, local.transpose(0, 2, 1)[:, :, None, :], 0.0), axis=-1)
    pick = pick.astype(BF16)

    x = jnp.einsum("sjkt,std->jskd", pick, normed, preferred_element_type=F32).astype(BF16)
    gate = jnp.einsum("jskd,jdf->jskf", x, w_gate, preferred_element_type=F32)
    up = jnp.einsum("jskd,jdf->jskf", x, w_up, preferred_element_type=F32)
    hidden = (jax.nn.silu(gate) * up).astype(BF16)
    y = jnp.einsum("jskf,jfd->jskd", hidden, w_down, preferred_element_type=F32)
    y = (y * slot_w.transpose(1, 0, 2)[..., None]).astype(BF16)
    routed = jnp.einsum("sjkt,jskd->std", pick, y, preferred_element_type=F32)

    own = lax.dynamic_index_in_dim(normed, me, 0, keepdims=False)
    sg = jnp.dot(own, shared_w_gate, preferred_element_type=F32)
    su = jnp.dot(own, shared_w_up, preferred_element_type=F32)
    sh = (jax.nn.silu(sg) * su).astype(BF16)
    part = jnp.dot(sh, shared_w_down, preferred_element_type=F32)
    share = jax.nn.sigmoid(jnp.dot(own, shared_gate_w, preferred_element_type=F32))
    part = share[:, None] * part
    mine = (jnp.arange(n_ep) == me)[:, None, None]
    total = (routed + jnp.where(mine, part[None], 0.0)).astype(BF16)
    total = total.reshape(n_ep, rows, n_tp, width)
    total = lax.psum_scatter(total, "tp", scatter_dimension=2, tiled=True)
    total = total.reshape(n_ep * rows, width)
    terms = lax.all_to_all(total, "ep", split_axis=0, concat_axis=0, tiled=True)
    return jnp.sum(terms.reshape(n_ep, rows, width).astype(F32), axis=0).astype(BF16)


def solution(mesh):
    def per_device(tokens, *rest):
        gathered = mesh.size * tokens.size * tokens.dtype.itemsize
        if gathered <= 16 << 20 and fits(mesh, tokens, *rest):
            return fused_plan(mesh, tokens, *rest)
        plan = gather_plan if gathered <= 16 << 20 else dispatch_plan
        return plan(tokens, *rest)

    return jax.shard_map(
        per_device,
        mesh=mesh,
        in_specs=(
            P("ep", "tp"),
            P(),
            P("tp", None),
            P(),
            P("ep", None),
            P("ep", None, "tp"),
            P("ep", None, "tp"),
            P("ep", "tp", None),
            P(None, "tp"),
            P(None, "tp"),
            P("tp", None),
        ),
        out_specs=P("ep", "tp"),
        check_vma=False,
    )
```
